32 devices in a mesh: tm: 8 (over z, y), space: 4 (over x, core).
Axes of the slice: x: 2, y: 2, z: 4, core: 2. Of those that a mesh axis runs over, the one named last changes fastest.
Arguments:
- start_values: float32 [8, 2, 1024, 1024], P('tm', None, 'space'), may hold values from -6 to 6
- node_values: float32 [8, 2, 2, 1024, 1024], P('tm', None, None, 'space'), may hold values from -6 to 6
Outputs:
- next_start: float32 [8, 2, 1024, 1024], P('tm', None, 'space')
- next_nodes: float32 [8, 2, 2, 1024, 1024], P('tm', None, None, 'space')
The draws below stay inside these ranges and needn't reach their ends.
All inputs are finite; a program needn't handle non-finite values.
Results may differ from the reference program's by a relative error of at most 0.00002.
Values sent between devices are 32-bit elements; how exact they have to be, the bound alone decides.
No kernel may reach another device: no remote copies, remote signals or barrier semaphores. Data moves between devices by JAX's collectives and lax.ppermute only.
A program may use at most 64 MiB of HBM per device.

```python
import jax
import jax.numpy as jnp
from jax import lax

KX = 1024
KY = 1024
CX = 256
NT = 8


def block_scale(stream_key, dims, shards, low, largest):
    loudness, own = 1.0, jax.random.fold_in(stream_key, 6)
    for dim, shards_of in shards:
        heights = jnp.exp(jax.random.uniform(jax.random.fold_in(own, dim), (shards_of,), jnp.float32, low / len(shards), largest / len(shards)))
        loudness = loudness * jnp.repeat(heights, dims[dim] // shards_of).reshape([-1 if axis == dim else 1 for axis in range(len(dims))])
    return loudness


def scatter_about(key, dims, width, reach, pieces=(), held_as=jnp.bfloat16):
    factor_of = block_scale(key, dims, pieces, -0.22, 0.18) if pieces else 1.0
    values = jax.random.normal(key, dims, jnp.float32) * width * factor_of
    return jnp.minimum(jnp.maximum(values, -reach), reach).astype(held_as)


def setup_inputs(seed: int = 0) -> dict:
    key_list = jax.random.split(jax.random.key(seed), 3)
    start_values = scatter_about(key_list[0], (NT, 2, KX, KY), 1.0, 6.0, ((0, 8), (2, 4)), jnp.float32)
    node_values = scatter_about(key_list[1], (NT, 2, 2, KX, KY), 1.0, 6.0, ((0, 8), (3, 4)), jnp.float32)
    return dict(start_values=start_values, node_values=node_values)


diffusion = 1.5
drift = 0.8
shear = 0.6
first_weights = (5.0 / 24.0, 1.0 / 3.0, -1.0 / 24.0)
second_weights = (-1.0 / 24.0, 1.0 / 3.0, 5.0 / 24.0)
whole_weights = (1.0 / 6.0, 2.0 / 3.0, 1.0 / 6.0)


def spectrum(row_index, column_index):
    along = (row_index.astype(jnp.float32) - KX // 2) / (KX // 2)
    across = (column_index.astype(jnp.float32) - KY // 2) / (KY // 2)
    real_rate = -diffusion * (along[:, None] * along[:, None] + across[None, :] * across[None, :])
    imag_rate = -drift * across[None, :] + 0.0 * along[:, None]
    return real_rate, imag_rate, across


def multiply(real_rate, imag_rate, field):
    return jnp.stack([real_rate * field[..., 0, :, :] - imag_rate * field[..., 1, :, :],
                      real_rate * field[..., 1, :, :] + imag_rate * field[..., 0, :, :]], axis=-3)


def divide(real_part, imag_part, field):
    modulus = real_part * real_part + imag_part * imag_part
    return jnp.stack([(field[..., 0, :, :] * real_part + field[..., 1, :, :] * imag_part) / modulus,
                      (field[..., 1, :, :] * real_part - field[..., 0, :, :] * imag_part) / modulus], axis=-3)


def coupling_of(padded, across):
    sums = padded[..., 2:, :] + padded[..., :-2, :]
    factor = shear * across
    return jnp.stack([factor * sums[..., 1, :, :], -factor * sums[..., 0, :, :]], axis=-3)


def explicit(field, across):
    widths = [(0, 0)] * (field.ndim - 2) + [(1, 1), (0, 0)]
    return coupling_of(jnp.pad(field, widths), across)


def fine_section(begin_value, old_nodes):
    real_rate, imag_rate, across = spectrum(jnp.arange(KX), jnp.arange(KY))
    stacked = jnp.stack([begin_value, old_nodes[0], old_nodes[1]])
    old_coupling = explicit(stacked, across)
    old_slopes = multiply(real_rate, imag_rate, stacked) + old_coupling
    sum_one = first_weights[0] * old_slopes[0] + first_weights[1] * old_slopes[1] + first_weights[2] * old_slopes[2]
    sum_two = second_weights[0] * old_slopes[0] + second_weights[1] * old_slopes[1] + second_weights[2] * old_slopes[2]
    half_real = 1.0 - 0.5 * real_rate
    half_imag = -0.5 * imag_rate
    node_one = divide(half_real, half_imag, begin_value - 0.5 * multiply(real_rate, imag_rate, old_nodes[0]) + sum_one)
    one_coupling = explicit(node_one[None], across)[0]
    node_two = divide(half_real, half_imag, node_one + 0.5 * (one_coupling - old_coupling[1])
                      - 0.5 * multiply(real_rate, imag_rate, old_nodes[1]) + sum_two)
    two_coupling = explicit(node_two[None], across)[0]
    integral = (whole_weights[0] * old_slopes[0]
                + whole_weights[1] * (multiply(real_rate, imag_rate, node_one) + one_coupling)
                + whole_weights[2] * (multiply(real_rate, imag_rate, node_two) + two_coupling))
    low_row = KX // 2 - CX // 2
    low_column = KY // 2 - CX // 2
    coarse_real = real_rate[low_row:low_row + CX, low_column:low_column + CX]
    coarse_imag = imag_rate[low_row:low_row + CX, low_column:low_column + CX]
    begin_coarse = begin_value[:, low_row:low_row + CX, low_column:low_column + CX]
    end_coarse = node_two[:, low_row:low_row + CX, low_column:low_column + CX]
    tau = integral[:, low_row:low_row + CX, low_column:low_column + CX] - 0.5 * multiply(coarse_real, coarse_imag, begin_coarse + end_coarse)
    offset = 0.5 * multiply(coarse_real, coarse_imag, begin_coarse - end_coarse) + tau
    return node_one, node_two, begin_coarse, end_coarse, offset


def reference(start_values, node_values):
    node_one, node_two, begin_coarse, end_coarse, offset = lax.map(
        lambda paired: fine_section(paired[0], paired[1]), (start_values, node_values))
    real_rate, imag_rate, across = spectrum(jnp.arange(KX), jnp.arange(KY))
    low_row = KX // 2 - CX // 2
    low_column = KY // 2 - CX // 2
    coarse_real = real_rate[low_row:low_row + CX, low_column:low_column + CX]
    coarse_imag = imag_rate[low_row:low_row + CX, low_column:low_column + CX]
    step_real = 1.0 - coarse_real
    step_imag = -coarse_imag
    coarse_starts = [begin_coarse[0]]
    for slice_index in range(1, NT):
        coarse_starts.append(divide(step_real, step_imag, coarse_starts[-1] + offset[slice_index - 1]))
    begin_new = jnp.stack(coarse_starts)
    end_new = divide(step_real, step_imag, begin_new + offset)
    delta_begin = begin_new - begin_coarse
    delta_end = end_new - end_coarse
    widths = ((0, 0), (0, 0), (low_row, KX - low_row - CX), (low_column, KY - low_column - CX))
    fixed_one = node_one + jnp.pad(0.5 * (delta_begin + delta_end), widths)
    fixed_two = node_two + jnp.pad(delta_end, widths)
    next_start = jnp.concatenate([start_values[:1], fixed_two[:-1]], axis=0)
    next_nodes = jnp.stack([fixed_one, fixed_two], axis=1)
    return (next_start, next_nodes)
```

```python
import functools

import jax
import jax.numpy as jnp
from jax import lax
from jax.experimental import pallas as pl
from jax.experimental.pallas import tpu as pltpu
from jax.sharding import PartitionSpec as P

COARSE_SHARE = 4
LANES = 128
STRIP = 32
HALO = 4
PAD = 8

diffusion = 1.5
drift = 0.8
shear = 0.6


def rates(row_start, rows, column_start, columns, size_x, size_y):
    row = row_start + lax.broadcasted_iota(jnp.int32, (rows, columns), 0)
    column = column_start + lax.broadcasted_iota(jnp.int32, (rows, columns), 1)
    along = (row.astype(jnp.float32) - size_x // 2) * (2.0 / size_x)
    across = (column.astype(jnp.float32) - size_y // 2) * (2.0 / size_y)
    real = -diffusion * (along * along + across * across)
    return real, -drift * across, shear * across


def turned(real, imag, first, second):
    return real * first - imag * second, real * second + imag * first


def fine_kernel(*refs, blocks, first_block, coarse, size_x, size_y, coarse_rows, pieces, aliased):
    begin, old, before, after = refs[:4]
    refs = refs[4 + aliased:]
    nodes, refs = refs[0], refs[1:]
    sends, refs = refs[: len(pieces)], refs[len(pieces):]
    offset = None
    if coarse:
        offset, refs = refs[0], refs[1:]
    wide_one, wide_two, inner, inverse = refs
    rows = begin.shape[1]
    rank = lax.axis_index("space")
    ranks = lax.axis_size("space")
    block = first_block + pl.program_id(0)
    row_base = rank * rows
    column_base = block * LANES
    has_before = rank > 0
    has_after = rank < ranks - 1
    tiles = [("in", start, min(STRIP, rows - start)) for start in range(0, rows, STRIP)]
    tiles = [("before", -HALO, HALO)] + tiles + [("after", rows, HALO)]

    def fields(kind, start, count):
        if kind == "in":
            here = pl.ds(start, count)
            return ([begin[0, here, :], begin[1, here, :]],
                    [old[0, 0, here, :], old[0, 1, here, :]],
                    [old[1, 0, here, :], old[1, 1, here, :]])
        side = before if kind == "before" else after
        return ([side[0], side[1]], [side[2], side[3]], [side[4], side[5]])

    def kept(kind, value):
        if kind == "before":
            return jnp.where(has_before, value, 0.0)
        if kind == "after":
            return jnp.where(has_after, value, 0.0)
        return value

    def sums(ref, part, start, count):
        return ref[part, pl.ds(PAD + start - 1, count), :] + ref[part, pl.ds(PAD + start + 1, count), :]

    for kind, start, count in tiles:
        b, one, two = fields(kind, start, count)
        for part in range(2):
            third = (1.0 / 3.0) * one[part]
            wide_one[part, pl.ds(PAD + start, count), :] = (5.0 / 24.0) * b[part] + third - (1.0 / 24.0) * two[part]
            wide_two[part, pl.ds(PAD + start, count), :] = third - (1.0 / 24.0) * b[part] + (5.0 / 24.0) * two[part] - 0.5 * one[part]
    for kind, start, count in tiles:
        real, imag, factor = rates(row_base + start, count, column_base, LANES, size_x, size_y)
        b, one, _ = fields(kind, start, count)
        here = pl.ds(PAD + start, count)
        u = [wide_one[part, here, :] - 0.5 * one[part] for part in range(2)]
        lu = turned(real, imag, u[0], u[1])
        top = (b[0] + lu[0] + factor * sums(wide_one, 1, start, count),
               b[1] + lu[1] - factor * sums(wide_one, 0, start, count))
        half_real = 1.0 - 0.5 * real
        half_imag = -0.5 * imag
        share = 1.0 / (half_real * half_real + half_imag * half_imag)
        half_real = half_real * share
        half_imag = half_imag * share
        inverse[0, here, :] = half_real
        inverse[1, here, :] = half_imag
        node = (top[0] * half_real + top[1] * half_imag, top[1] * half_real - top[0] * half_imag)
        for part in range(2):
            value = kept(kind, node[part])
            if kind == "in":
                nodes[0, part, pl.ds(start, count), :] = value
            inner[part, here, :] = value
    for kind, start, count in tiles:
        here = pl.ds(PAD + start, count)
        for part in range(2):
            wide_one[part, here, :] = 0.5 * inner[part, here, :] + wide_two[part, here, :]
    for kind, start, count in tiles:
        if kind != "in" and not coarse:
            continue
        real, imag, factor = rates(row_base + start, count, column_base, LANES, size_x, size_y)
        b, one, two = fields(kind, start, count)
        here = pl.ds(PAD + start, count)
        u = [wide_two[part, here, :] + 0.5 * (one[part] - two[part]) for part in range(2)]
        lu = turned(real, imag, u[0], u[1])
        n1 = [inner[part, here, :] for part in range(2)]
        top = (n1[0] + lu[0] + factor * sums(wide_one, 1, start, count),
               n1[1] + lu[1] - factor * sums(wide_one, 0, start, count))
        half_real = inverse[0, here, :]
        half_imag = inverse[1, here, :]
        node = (top[0] * half_real + top[1] * half_imag, top[1] * half_real - top[0] * half_imag)
        for part in range(2):
            value = kept(kind, node[part])
            if kind == "in":
                nodes[1, part, pl.ds(start, count), :] = value
                for (low, high), send in zip(pieces, sends):
                    a, z = max(low, start), min(high, start + count)
                    if a < z:
                        send[part, pl.ds(a - low, z - a), :] = value[a - start:z - start]
            if coarse:
                inner[part, here, :] = (1.0 / 6.0) * b[part] + (2.0 / 3.0) * n1[part] + (1.0 / 6.0) * value
    if coarse:
        def offsets(shift):
            for start in range(0, coarse_rows, STRIP):
                count = min(STRIP, coarse_rows - start)
                at = shift + start
                real, imag, factor = rates(row_base + at, count, column_base, LANES, size_x, size_y)
                v = [inner[part, pl.ds(PAD + at, count), :] for part in range(2)]
                e = [nodes[1, part, pl.ds(at, count), :] for part in range(2)]
                lu = turned(real, imag, v[0] - e[0], v[1] - e[1])
                off = (lu[0] + factor * sums(inner, 1, at, count),
                       lu[1] - factor * sums(inner, 0, at, count))
                step_real = 1.0 - real
                step_imag = -imag
                share = 1.0 / (step_real * step_real + step_imag * step_imag)
                lead = lax.axis_index("tm") == 0
                off = tuple(off[part] + jnp.where(lead, begin[part, pl.ds(at, count), :], 0.0) for part in range(2))
                offset[0, pl.ds(start, count), :] = (off[0] * step_real + off[1] * step_imag) * share
                offset[1, pl.ds(start, count), :] = (off[1] * step_real - off[0] * step_imag) * share

        low_shift = rows - coarse_rows
        if low_shift == 0:
            offsets(0)
        else:
            upper = rank >= ranks // 2

            @pl.when(upper)
            def _():
                offsets(0)

            @pl.when(jnp.logical_not(upper))
            def _():
                offsets(low_shift)


def fine_call(begin, old, before, after, nodes, first, width, coarse, pieces, size_x, coarse_rows):
    rows, columns = begin.shape[1:]
    blocks = width // LANES
    base = first // LANES
    f32 = jnp.float32
    out_shape = [jax.ShapeDtypeStruct((2, 2, rows, columns), f32)]
    out_specs = [pl.BlockSpec((2, 2, rows, LANES), lambda j: (0, 0, 0, base + j))]
    for low, high in pieces:
        out_shape.append(jax.ShapeDtypeStruct((2, high - low, width), f32))
        out_specs.append(pl.BlockSpec((2, high - low, LANES), lambda j: (0, 0, j)))
    if coarse:
        out_shape.append(jax.ShapeDtypeStruct((2, coarse_rows, width), f32))
        out_specs.append(pl.BlockSpec((2, coarse_rows, LANES), lambda j: (0, 0, j)))
    in_specs = [
        pl.BlockSpec((2, rows, LANES), lambda j: (0, 0, base + j)),
        pl.BlockSpec((2, 2, rows, LANES), lambda j: (0, 0, 0, base + j)),
        pl.BlockSpec((6, HALO, LANES), lambda j: (0, 0, base + j)),
        pl.BlockSpec((6, HALO, LANES), lambda j: (0, 0, base + j)),
    ]
    operands = [begin, old, before, after]
    aliases = {}
    if nodes is not None:
        operands.append(nodes)
        in_specs.append(pl.BlockSpec(memory_space=pl.ANY))
        aliases = {4: 0}
    kernel = functools.partial(
        fine_kernel, blocks=blocks, first_block=base, coarse=coarse, size_x=size_x, size_y=columns,
        coarse_rows=coarse_rows, pieces=pieces, aliased=len(aliases))
    scratch = [pltpu.VMEM((2, rows + 2 * PAD, LANES), f32) for _ in range(4)]
    return pl.pallas_call(
        kernel, grid=(blocks,), in_specs=in_specs, out_specs=out_specs, out_shape=out_shape,
        scratch_shapes=scratch, input_output_aliases=aliases, name="fine_coarse" if coarse else "fine",
    )(*operands)


def place_kernel(*refs, targets, patch, aliased, coarse_rows, low_column):
    count = len(targets)
    begin = refs[0]
    arrived = refs[1:1 + count]
    refs = refs[1 + count:]
    rank = lax.axis_index("space")
    ranks = lax.axis_size("space")
    lead = lax.axis_index("tm") == 0
    if patch:
        fresh, finish = refs[:2]
        refs = refs[3 + aliased:]
        start, nodes, sems, block_begin, block_nodes, fixed = refs
    else:
        start, sems = refs[aliased:]
    rows = begin.shape[1]
    if patch:
        shift = jnp.where(rank >= ranks // 2, 0, rows - coarse_rows)
        middle = jnp.logical_or(rank == ranks // 2, rank == ranks // 2 - 1)
        shift = pl.multiple_of(shift, 8)
        width = fresh.shape[2]
        spot = (slice(None), pl.ds(shift, coarse_rows), pl.ds(low_column, width))
        loads = [pltpu.make_async_copy(begin.at[spot], block_begin, sems.at[count]),
                 pltpu.make_async_copy(nodes.at[(slice(None),) + spot], block_nodes, sems.at[count + 1])]

        @pl.when(middle)
        def _():
            for copy in loads:
                copy.start()

    copies = []
    for k, (low, high, first, width_k, skip) in enumerate(targets):
        where = (slice(None), pl.ds(low, high - low), pl.ds(first, width_k))
        own = pltpu.make_async_copy(begin.at[where], start.at[where], sems.at[k])
        moved = pltpu.make_async_copy(arrived[k], start.at[where], sems.at[k])
        live = jnp.bool_(True)
        for other in skip:
            live = jnp.logical_and(live, rank != other)
        copies.append((own, moved, live))

        @pl.when(lead)
        def _():
            own.start()

        @pl.when(jnp.logical_and(jnp.logical_not(lead), live))
        def _():
            moved.start()

    if patch:
        @pl.when(middle)
        def _():
            for copy in loads:
                copy.wait()
            for part in range(2):
                old_begin = block_begin[part]
                n1 = block_nodes[0, part]
                n2 = block_nodes[1, part]
                now = jnp.where(lead, old_begin, fresh[part])
                end = finish[part]
                change = end - n2
                fixed[0, part] = n1 + 0.5 * ((now - old_begin) + change)
                fixed[1, part] = n2 + change
                block_begin[part] = now
            store = pltpu.make_async_copy(fixed, nodes.at[(slice(None),) + spot], sems.at[count])
            store.start()

            @pl.when(jnp.logical_not(lead))
            def _():
                put = pltpu.make_async_copy(block_begin, start.at[spot], sems.at[count + 1])
                put.start()
                put.wait()

            store.wait()

    for own, moved, live in copies:
        @pl.when(jnp.logical_or(lead, live))
        def _():
            own.wait()


def place_call(begin, arrived, targets, start, coarse_part, nodes, coarse_rows, low_column):
    f32 = jnp.float32
    anywhere = pl.BlockSpec(memory_space=pl.ANY)
    vmem = pl.BlockSpec(memory_space=pltpu.VMEM)
    operands = [begin] + list(arrived)
    in_specs = [anywhere] * len(operands)
    out_shape = [jax.ShapeDtypeStruct(begin.shape, f32)]
    out_specs = [anywhere]
    scratch = []
    aliases = {}
    patch = coarse_part is not None
    if patch:
        operands += list(coarse_part) + [nodes]
        in_specs += [vmem, vmem, anywhere]
        out_shape.append(jax.ShapeDtypeStruct(nodes.shape, f32))
        out_specs.append(anywhere)
        aliases[len(operands) - 1] = 1
        block = (2,) + coarse_part[0].shape[1:]
        scratch = [pltpu.VMEM(block, f32), pltpu.VMEM((2,) + block, f32), pltpu.VMEM((2,) + block, f32)]
    aliased = 0
    if start is not None:
        aliases[len(operands)] = 0
        operands.append(start)
        in_specs.append(anywhere)
        aliased = 1
    kernel = functools.partial(place_kernel, targets=targets, patch=patch, aliased=aliased,
                               coarse_rows=coarse_rows, low_column=low_column)
    return pl.pallas_call(
        kernel, in_specs=in_specs, out_specs=out_specs, out_shape=out_shape,
        scratch_shapes=[pltpu.SemaphoreType.DMA((len(targets) + 2,))] + scratch,
        input_output_aliases=aliases, name="place_patch" if patch else "place",
    )(*operands)


def powers(row_base, rows, low_column, width, size_x, size_y):
    real, imag, _ = rates(row_base, rows, low_column, width, size_x, size_y)
    step_real = 1.0 - real
    step_imag = -imag
    share = 1.0 / (step_real * step_real + step_imag * step_imag)
    return step_real * share, -step_imag * share


def body(start_values, node_values):
    begin = start_values[0]
    old = node_values[0]
    rows, columns = begin.shape[1:]
    slices, ranks = lax.axis_size("tm"), lax.axis_size("space")
    size_x = rows * ranks
    width = columns // COARSE_SHARE
    low_column = columns // 2 - width // 2
    coarse_rows = min(rows, size_x // COARSE_SHARE // 2)
    lower, upper = ranks // 2 - 1, ranks // 2
    rank = lax.axis_index("space")
    lead = lax.axis_index("tm") == 0

    def edge(low):
        cut = [begin[:, low:low + HALO], old[0, :, low:low + HALO], old[1, :, low:low + HALO]]
        return jnp.concatenate(cut, axis=0)

    up = [(i, i + 1) for i in range(ranks - 1)]
    before = lax.ppermute(edge(rows - HALO), "space", up)
    after = lax.ppermute(edge(0), "space", [(j, i) for i, j in up])

    def ahead(value, steps, members):
        pairs = [(n * ranks + s, (n + steps) * ranks + s) for n in range(slices - steps) for s in members]
        return lax.ppermute(value, ("tm", "space"), pairs)

    everyone = range(ranks)
    middle = (lower, upper)
    if rows == coarse_rows:
        pieces = [(0, rows)]
        holders = [[s for s in everyone if s not in middle]]
    else:
        cuts = [0, coarse_rows, rows - coarse_rows, rows]
        pieces = [(a, b) for a, b in zip(cuts, cuts[1:]) if a < b]
        holders = [[s for s in everyone
                    if not (s == upper and b <= coarse_rows) and not (s == lower and a >= rows - coarse_rows)]
                   for a, b in pieces]
    made = fine_call(begin, old, before, after, None, low_column, width, True, pieces, size_x, coarse_rows)
    nodes, inner_sends, offset = made[0], made[1:-1], made[-1]
    one_back = ahead(offset, 1, middle)
    two_back = ahead(offset, 2, middle)
    rest = columns - low_column - width
    nodes, left = fine_call(begin, old, before, after, nodes, 0, low_column, False, [(0, rows)], size_x, coarse_rows)
    left = ahead(left, 1, everyone)
    nodes, right = fine_call(begin, old, before, after, nodes, low_column + width, rest, False, [(0, rows)], size_x, coarse_rows)

    shift = jnp.where(rank >= ranks // 2, 0, rows - coarse_rows)
    d_real, d_imag = powers(rank * rows + shift, coarse_rows, low_column, width, size_x, columns)

    def add(total, field, real, imag):
        grown = turned(real, imag, field[0], field[1])
        return jnp.stack([total[0] + grown[0], total[1] + grown[1]])

    total = add(one_back, two_back, d_real, d_imag)
    inner = [ahead(piece, 1, members) for piece, members in zip(inner_sends, holders)]
    right = ahead(right, 1, everyone)
    power = turned(d_real, d_imag, d_real, d_imag)
    reach = 2
    while reach < slices:
        total = add(total, ahead(total, reach, middle), *power)
        power = turned(power[0], power[1], power[0], power[1])
        reach *= 2
    end = add(offset, jnp.where(lead, 0.0, total), d_real, d_imag)
    targets = [(a, b, low_column, width, tuple(s for s in everyone if s not in members))
               for (a, b), members in zip(pieces, holders)]
    arrived = list(inner)
    targets.append((0, rows, 0, low_column, ()))
    arrived.append(left)
    next_start, nodes = place_call(begin, arrived, targets, None, (total, end), nodes, coarse_rows, low_column)
    (next_start,) = place_call(begin, [right], [(0, rows, low_column + width, rest, ())], next_start,
                               None, None, coarse_rows, low_column)
    return next_start[None], nodes[None]


def solution(mesh):
    in_specs = (P("tm", None, "space", None), P("tm", None, None, "space", None))
    out_specs = (P("tm", None, "space", None), P("tm", None, None, "space", None))
    return jax.shard_map(body, mesh=mesh, in_specs=in_specs, out_specs=out_specs, check_vma=False)
```

```python
import functools

import jax
import jax.numpy as jnp
from jax import lax
from jax.experimental import pallas as pl
from jax.experimental.pallas import tpu as pltpu
from jax.sharding import PartitionSpec as P

COARSE_SHARE = 4
LANES = 128
STRIP = 32
HALO = 4
PAD = 8

diffusion = 1.5
drift = 0.8
shear = 0.6


def rates(row_start, rows, column_start, columns, size_x, size_y):
    row = row_start + lax.broadcasted_iota(jnp.int32, (rows, columns), 0)
    column = column_start + lax.broadcasted_iota(jnp.int32, (rows, columns), 1)
    along = (row.astype(jnp.float32) - size_x // 2) * (2.0 / size_x)
    across = (column.astype(jnp.float32) - size_y // 2) * (2.0 / size_y)
    real = -diffusion * (along * along + across * across)
    return real, -drift * across, shear * across


def turned(real, imag, first, second):
    return real * first - imag * second, real * second + imag * first


def fine_kernel(*refs, first_block, coarse, size_x, size_y, coarse_rows, pieces, aliased):
    begin, old = refs[:2]
    refs = refs[2:]
    if coarse:
        before, after = refs[:2]
        refs = refs[2:]
    refs = refs[aliased:]
    nodes, refs = refs[0], refs[1:]
    sends, refs = refs[: len(pieces)], refs[len(pieces):]
    offset = None
    if coarse:
        offset, refs = refs[0], refs[1:]
    wide_one, wide_two, inner, inverse = refs
    rows = begin.shape[1]
    rank = lax.axis_index("space")
    ranks = lax.axis_size("space")
    spot = pl.ds(pl.multiple_of(pl.program_id(0) * LANES, LANES), LANES)
    row_base = rank * rows
    column_base = (first_block + pl.program_id(0)) * LANES
    has_before = rank > 0
    has_after = rank < ranks - 1
    tiles = [("in", start, min(STRIP, rows - start)) for start in range(0, rows, STRIP)]
    if coarse:
        whole = pl.ds((first_block + pl.program_id(0)) * LANES, LANES)
        tiles = [("before", -HALO, HALO)] + tiles + [("after", rows, HALO)]

    def fields(kind, start, count):
        if kind == "in":
            here = pl.ds(start, count)
            return ([begin[0, here, :], begin[1, here, :]],
                    [old[0, 0, here, :], old[0, 1, here, :]],
                    [old[1, 0, here, :], old[1, 1, here, :]])
        side = before if kind == "before" else after
        part = [side[k, :, whole] for k in range(6)]
        return (part[:2], part[2:4], part[4:])

    def kept(kind, value):
        if kind == "before":
            return jnp.where(has_before, value, 0.0)
        if kind == "after":
            return jnp.where(has_after, value, 0.0)
        return value

    def sums(ref, part, start, count):
        return ref[part, pl.ds(PAD + start - 1, count), :] + ref[part, pl.ds(PAD + start + 1, count), :]

    for kind, start, count in tiles:
        b, one, two = fields(kind, start, count)
        for part in range(2):
            third = (1.0 / 3.0) * one[part]
            wide_one[part, pl.ds(PAD + start, count), :] = (5.0 / 24.0) * b[part] + third - (1.0 / 24.0) * two[part]
            wide_two[part, pl.ds(PAD + start, count), :] = third - (1.0 / 24.0) * b[part] + (5.0 / 24.0) * two[part] - 0.5 * one[part]
    for kind, start, count in tiles:
        real, imag, factor = rates(row_base + start, count, column_base, LANES, size_x, size_y)
        b, one, _ = fields(kind, start, count)
        here = pl.ds(PAD + start, count)
        u = [wide_one[part, here, :] - 0.5 * one[part] for part in range(2)]
        lu = turned(real, imag, u[0], u[1])
        top = (b[0] + lu[0] + factor * sums(wide_one, 1, start, count),
               b[1] + lu[1] - factor * sums(wide_one, 0, start, count))
        half_real = 1.0 - 0.5 * real
        half_imag = -0.5 * imag
        share = 1.0 / (half_real * half_real + half_imag * half_imag)
        half_real = half_real * share
        half_imag = half_imag * share
        inverse[0, here, :] = half_real
        inverse[1, here, :] = half_imag
        node = (top[0] * half_real + top[1] * half_imag, top[1] * half_real - top[0] * half_imag)
        for part in range(2):
            value = kept(kind, node[part])
            if kind == "in":
                nodes[0, part, pl.ds(start, count), :] = value
            inner[part, here, :] = value
    for kind, start, count in tiles:
        here = pl.ds(PAD + start, count)
        for part in range(2):
            wide_one[part, here, :] = 0.5 * inner[part, here, :] + wide_two[part, here, :]
    for kind, start, count in tiles:
        if kind != "in" and not coarse:
            continue
        real, imag, factor = rates(row_base + start, count, column_base, LANES, size_x, size_y)
        b, one, two = fields(kind, start, count)
        here = pl.ds(PAD + start, count)
        u = [wide_two[part, here, :] + 0.5 * (one[part] - two[part]) for part in range(2)]
        lu = turned(real, imag, u[0], u[1])
        n1 = [inner[part, here, :] for part in range(2)]
        top = (n1[0] + lu[0] + factor * sums(wide_one, 1, start, count),
               n1[1] + lu[1] - factor * sums(wide_one, 0, start, count))
        half_real = inverse[0, here, :]
        half_imag = inverse[1, here, :]
        node = (top[0] * half_real + top[1] * half_imag, top[1] * half_real - top[0] * half_imag)
        for part in range(2):
            value = kept(kind, node[part])
            if kind == "in":
                nodes[1, part, pl.ds(start, count), :] = value
                for (low, high), send in zip(pieces, sends):
                    a, z = max(low, start), min(high, start + count)
                    if a < z:
                        send[part, pl.ds(a - low, z - a), spot] = value[a - start:z - start]
            if coarse:
                inner[part, here, :] = (1.0 / 6.0) * b[part] + (2.0 / 3.0) * n1[part] + (1.0 / 6.0) * value
    if coarse:
        def offsets(shift):
            for start in range(0, coarse_rows, STRIP):
                count = min(STRIP, coarse_rows - start)
                at = shift + start
                real, imag, factor = rates(row_base + at, count, column_base, LANES, size_x, size_y)
                v = [inner[part, pl.ds(PAD + at, count), :] for part in range(2)]
                e = [nodes[1, part, pl.ds(at, count), :] for part in range(2)]
                lu = turned(real, imag, v[0] - e[0], v[1] - e[1])
                off = (lu[0] + factor * sums(inner, 1, at, count),
                       lu[1] - factor * sums(inner, 0, at, count))
                step_real = 1.0 - real
                step_imag = -imag
                share = 1.0 / (step_real * step_real + step_imag * step_imag)
                lead = lax.axis_index("tm") == 0
                off = tuple(off[part] + jnp.where(lead, begin[part, pl.ds(at, count), :], 0.0) for part in range(2))
                offset[0, pl.ds(start, count), spot] = (off[0] * step_real + off[1] * step_imag) * share
                offset[1, pl.ds(start, count), spot] = (off[1] * step_real - off[0] * step_imag) * share

        low_shift = rows - coarse_rows
        if low_shift == 0:
            offsets(0)
        else:
            upper = rank >= ranks // 2

            @pl.when(upper)
            def _():
                offsets(0)

            @pl.when(jnp.logical_not(upper))
            def _():
                offsets(low_shift)


VMEM = pl.BlockSpec(memory_space=pltpu.VMEM)
ANY = pl.BlockSpec(memory_space=pl.ANY)
PARAMS = pltpu.CompilerParams(vmem_limit_bytes=28 * 1024 * 1024)


def fine_call(begin, old, halo, nodes, first, width, pieces, size_x, coarse_rows):
    rows, columns = begin.shape[1:]
    coarse = halo is not None
    base = first // LANES
    f32 = jnp.float32
    out_shape = [jax.ShapeDtypeStruct((2, 2, rows, columns), f32)]
    out_specs = [pl.BlockSpec((2, 2, rows, LANES), lambda j: (0, 0, 0, base + j))]
    for low, high in pieces:
        out_shape.append(jax.ShapeDtypeStruct((2, high - low, width), f32))
        out_specs.append(VMEM)
    if coarse:
        out_shape.append(jax.ShapeDtypeStruct((2, coarse_rows, width), f32))
        out_specs.append(VMEM)
    in_specs = [
        pl.BlockSpec((2, rows, LANES), lambda j: (0, 0, base + j)),
        pl.BlockSpec((2, 2, rows, LANES), lambda j: (0, 0, 0, base + j)),
    ]
    operands = [begin, old]
    if coarse:
        operands += list(halo)
        in_specs += [VMEM, VMEM]
    aliases = {}
    if nodes is not None:
        aliases = {len(operands): 0}
        operands.append(nodes)
        in_specs.append(ANY)
    kernel = functools.partial(
        fine_kernel, first_block=base, coarse=coarse, size_x=size_x, size_y=columns,
        coarse_rows=coarse_rows, pieces=pieces, aliased=len(aliases))
    scratch = [pltpu.VMEM((2, rows + 2 * PAD, LANES), f32) for _ in range(4)]
    return pl.pallas_call(
        kernel, grid=(width // LANES,), in_specs=in_specs, out_specs=out_specs, out_shape=out_shape,
        scratch_shapes=scratch, input_output_aliases=aliases, compiler_params=PARAMS,
        name="fine_coarse" if coarse else "fine",
    )(*operands)


def edge_kernel(begin_top, old_top, begin_end, old_end, before, after, _, nodes, send, wide, fixed, sems,
                *, rows, size_x, size_y, outer):
    rank = lax.axis_index("space")
    ranks = lax.axis_size("space")
    side_rows = begin_top.shape[1]
    height = HALO + side_rows
    copies = []
    for k, (low, width, spot) in enumerate(outer):
        cut = pl.ds(low, width)
        for top in (True, False):
            begin, old, halo = (begin_top, old_top, before) if top else (begin_end, old_end, after)
            base = rank * rows + (-HALO if top else rows - side_rows)

            def field(index):
                if index < 2:
                    near = begin[index, :, cut]
                else:
                    near = old[index // 2 - 1, index % 2, :, cut]
                far = halo[index, :, cut]
                return jnp.concatenate([far, near] if top else [near, far], axis=0)

            real, imag, factor = rates(base, height, low, width, size_x, size_y)
            b, one, two = [[field(2 * k + part) for part in range(2)] for k in range(3)]

            def coupled(pair):
                moved = []
                for part in range(2):
                    wide[part, pl.ds(PAD, height), :] = pair[part]
                    moved.append(wide[part, pl.ds(PAD - 1, height), :] + wide[part, pl.ds(PAD + 1, height), :])
                return factor * moved[1], -factor * moved[0]

            half_real = 1.0 - 0.5 * real
            half_imag = -0.5 * imag
            share = 1.0 / (half_real * half_real + half_imag * half_imag)

            def divided(x, y):
                return (x * half_real + y * half_imag) * share, (y * half_real - x * half_imag) * share

            w1 = [(5.0 / 24.0) * b[p] + (1.0 / 3.0) * one[p] - (1.0 / 24.0) * two[p] for p in range(2)]
            w2 = [(1.0 / 3.0) * one[p] - (1.0 / 24.0) * b[p] + (5.0 / 24.0) * two[p] for p in range(2)]
            lu = turned(real, imag, w1[0] - 0.5 * one[0], w1[1] - 0.5 * one[1])
            cw = coupled(w1)
            n1 = divided(b[0] + lu[0] + cw[0], b[1] + lu[1] + cw[1])
            row = base + lax.broadcasted_iota(jnp.int32, (height, width), 0)
            inside = jnp.logical_and(row >= 0, row < size_x)
            n1 = [jnp.where(inside, value, 0.0) for value in n1]
            cw = coupled([0.5 * (n1[p] - one[p]) + w2[p] for p in range(2)])
            lu = turned(real, imag, w2[0] - 0.5 * two[0], w2[1] - 0.5 * two[1])
            n2 = divided(n1[0] + lu[0] + cw[0], n1[1] + lu[1] + cw[1])
            keep = slice(HALO, HALO + PAD) if top else slice(side_rows - PAD, side_rows)
            at = 0 if top else PAD
            for part in range(2):
                fixed[0, part, pl.ds(at, PAD), pl.ds(spot, width)] = n1[part][keep]
                fixed[1, part, pl.ds(at, PAD), pl.ds(spot, width)] = n2[part][keep]
                send[part, pl.ds(at, PAD), pl.ds(spot, width)] = n2[part][keep]
            copy = pltpu.make_async_copy(
                fixed.at[:, :, pl.ds(at, PAD), pl.ds(spot, width)],
                nodes.at[:, :, pl.ds(0 if top else rows - PAD, PAD), cut], sems.at[2 * k + (not top)])
            copy.start()
            copies.append(copy)
    for copy in copies:
        copy.wait()


def edge_call(begin, old, halo, nodes, outer, size_x):
    rows, columns = begin.shape[1:]
    side = 2 * PAD
    last = rows // side - 1
    total = sum(width for _, width in outer)
    f32 = jnp.float32
    spots, at = [], 0
    for low, width in outer:
        spots.append((low, width, at))
        at += width
    widest = max(width for _, width in outer)
    assert all(width == widest for _, width in outer)
    kernel = functools.partial(edge_kernel, rows=rows, size_x=size_x, size_y=columns, outer=spots)
    return pl.pallas_call(
        kernel, grid=(1,),
        in_specs=[pl.BlockSpec((2, side, columns), lambda j: (0, 0, 0)),
                  pl.BlockSpec((2, 2, side, columns), lambda j: (0, 0, 0, 0)),
                  pl.BlockSpec((2, side, columns), lambda j: (0, last, 0)),
                  pl.BlockSpec((2, 2, side, columns), lambda j: (0, 0, last, 0)),
                  VMEM, VMEM, ANY],
        out_specs=[ANY, VMEM],
        out_shape=[jax.ShapeDtypeStruct(nodes.shape, f32), jax.ShapeDtypeStruct((2, side, total), f32)],
        scratch_shapes=[pltpu.VMEM((2, 2 * PAD + HALO + side + PAD, widest), f32),
                        pltpu.VMEM((2, 2, side, total), f32), pltpu.SemaphoreType.DMA((2 * len(outer),))],
        input_output_aliases={6: 0}, compiler_params=PARAMS, name="edges",
    )(begin, old, begin, old, halo[0], halo[1], nodes)


def patch_kernel(*refs, count, pieces, coarse_rows):
    begin, nodes_in = refs[:2]
    arrived = refs[2:2 + count]
    fresh, finish, start, nodes = refs[2 + count:]
    rows = begin.shape[1]
    rank = lax.axis_index("space")
    ranks = lax.axis_size("space")
    lead = lax.axis_index("tm") == 0
    spot = pl.ds(pl.multiple_of(pl.program_id(0) * LANES, LANES), LANES)
    middle = jnp.logical_or(rank == ranks // 2, rank == ranks // 2 - 1)
    for (low, high), piece in zip(pieces, arrived):
        here = pl.ds(low, high - low)
        for part in range(2):
            start[part, here, :] = jnp.where(lead, begin[part, here, :], piece[part, :, spot])
    nodes[...] = nodes_in[...]

    def fix(shift):
        here = pl.ds(shift, coarse_rows)
        for part in range(2):
            old_begin = begin[part, here, :]
            n2 = nodes_in[1, part, here, :]
            now = jnp.where(lead, old_begin, fresh[part, :, spot])
            change = finish[part, :, spot] - n2
            nodes[0, part, here, :] = nodes_in[0, part, here, :] + 0.5 * ((now - old_begin) + change)
            nodes[1, part, here, :] = n2 + change
            start[part, here, :] = now

    if rows == coarse_rows:
        @pl.when(middle)
        def _():
            fix(0)
    else:
        @pl.when(rank == ranks // 2)
        def _():
            fix(0)

        @pl.when(rank == ranks // 2 - 1)
        def _():
            fix(rows - coarse_rows)


def patch_call(begin, nodes, arrived, pieces, fresh, finish, low_column, coarse_rows):
    rows = begin.shape[1]
    base = low_column // LANES
    begin_spec = pl.BlockSpec((2, rows, LANES), lambda j: (0, 0, base + j))
    nodes_spec = pl.BlockSpec((2, 2, rows, LANES), lambda j: (0, 0, 0, base + j))
    kernel = functools.partial(patch_kernel, count=len(arrived), pieces=pieces, coarse_rows=coarse_rows)
    return pl.pallas_call(
        kernel, grid=(fresh.shape[2] // LANES,),
        in_specs=[begin_spec, nodes_spec] + [VMEM] * (len(arrived) + 2),
        out_specs=[begin_spec, nodes_spec],
        out_shape=[jax.ShapeDtypeStruct(begin.shape, jnp.float32), jax.ShapeDtypeStruct(nodes.shape, jnp.float32)],
        input_output_aliases={1: 1}, compiler_params=PARAMS, name="patch",
    )(begin, nodes, *arrived, fresh, finish)


def place_kernel(begin, middle, edges, _, start, *, spot):
    lead = lax.axis_index("tm") == 0
    rows = begin.shape[1]
    here = pl.ds(pl.multiple_of(pl.program_id(0) * LANES, LANES), LANES)
    side = pl.ds(pl.multiple_of(spot + pl.program_id(0) * LANES, LANES), LANES)
    for part in range(2):
        start[part, pl.ds(0, PAD), :] = jnp.where(lead, begin[part, pl.ds(0, PAD), :], edges[part, pl.ds(0, PAD), side])
        start[part, pl.ds(PAD, rows - 2 * PAD), :] = jnp.where(
            lead, begin[part, pl.ds(PAD, rows - 2 * PAD), :], middle[part, :, here])
        start[part, pl.ds(rows - PAD, PAD), :] = jnp.where(
            lead, begin[part, pl.ds(rows - PAD, PAD), :], edges[part, pl.ds(PAD, PAD), side])


def place_call(begin, middle, edges, start, first, spot):
    rows = begin.shape[1]
    base = first // LANES
    spec = pl.BlockSpec((2, rows, LANES), lambda j: (0, 0, base + j))
    return pl.pallas_call(
        functools.partial(place_kernel, spot=spot), grid=(middle.shape[2] // LANES,),
        in_specs=[spec, VMEM, VMEM, ANY], out_specs=spec,
        out_shape=jax.ShapeDtypeStruct(begin.shape, jnp.float32),
        input_output_aliases={3: 0}, compiler_params=PARAMS, name="place",
    )(begin, middle, edges, start)


def powers(row_base, rows, low_column, width, size_x, size_y):
    real, imag, _ = rates(row_base, rows, low_column, width, size_x, size_y)
    step_real = 1.0 - real
    step_imag = -imag
    share = 1.0 / (step_real * step_real + step_imag * step_imag)
    return step_real * share, -step_imag * share


def body(start_values, node_values):
    begin = start_values[0]
    old = node_values[0]
    rows, columns = begin.shape[1:]
    slices, ranks = lax.axis_size("tm"), lax.axis_size("space")
    size_x = rows * ranks
    width = columns // COARSE_SHARE
    low_column = columns // 2 - width // 2
    coarse_rows = min(rows, size_x // COARSE_SHARE // 2)
    lower, upper = ranks // 2 - 1, ranks // 2
    rank = lax.axis_index("space")
    lead = lax.axis_index("tm") == 0

    def edge(low):
        cut = [begin[:, low:low + HALO], old[0, :, low:low + HALO], old[1, :, low:low + HALO]]
        return jnp.concatenate(cut, axis=0)

    up = [(i, i + 1) for i in range(ranks - 1)]
    before = lax.ppermute(edge(rows - HALO), "space", up)
    after = lax.ppermute(edge(0), "space", [(j, i) for i, j in up])

    def ahead(value, steps, members):
        pairs = [(n * ranks + s, (n + steps) * ranks + s) for n in range(slices - steps) for s in members]
        return lax.ppermute(value, ("tm", "space"), pairs)

    everyone = range(ranks)
    middle = (lower, upper)
    if rows == coarse_rows:
        pieces = [(0, rows)]
        holders = [[s for s in everyone if s not in middle]]
    else:
        cuts = [0, coarse_rows, rows - coarse_rows, rows]
        pieces = [(a, b) for a, b in zip(cuts, cuts[1:]) if a < b]
        holders = [[s for s in everyone
                    if not (s == upper and b <= coarse_rows) and not (s == lower and a >= rows - coarse_rows)]
                   for a, b in pieces]
    second = low_column + width
    rest = columns - second
    inside = [(PAD, rows - PAD)]
    nodes, left = fine_call(begin, old, None, None, 0, low_column, inside, size_x, coarse_rows)
    left = ahead(left, 1, everyone)
    nodes, right = fine_call(begin, old, None, nodes, second, rest, inside, size_x, coarse_rows)
    made = fine_call(begin, old, (before, after), nodes, low_column, width, pieces, size_x, coarse_rows)
    nodes, inner_sends, offset = made[0], made[1:-1], made[-1]
    one_back = ahead(offset, 1, middle)
    two_back = ahead(offset, 2, middle)
    right = ahead(right, 1, everyone)
    nodes, edges = edge_call(begin, old, (before, after), nodes, [(0, low_column), (second, rest)], size_x)
    edges = ahead(edges, 1, everyone)

    shift = jnp.where(rank >= ranks // 2, 0, rows - coarse_rows)
    d_real, d_imag = powers(rank * rows + shift, coarse_rows, low_column, width, size_x, columns)

    def add(total, field, real, imag):
        grown = turned(real, imag, field[0], field[1])
        return jnp.stack([total[0] + grown[0], total[1] + grown[1]])

    total = add(one_back, two_back, d_real, d_imag)
    inner = [ahead(piece, 1, members) for piece, members in zip(inner_sends, holders)]
    power = turned(d_real, d_imag, d_real, d_imag)
    reach = 2
    while reach < slices:
        total = add(total, ahead(total, reach, middle), *power)
        power = turned(power[0], power[1], power[0], power[1])
        reach *= 2
    end = add(offset, jnp.where(lead, 0.0, total), d_real, d_imag)
    next_start, nodes = patch_call(begin, nodes, inner, pieces, total, end, low_column, coarse_rows)
    next_start = place_call(begin, left, edges, next_start, 0, 0)
    next_start = place_call(begin, right, edges, next_start, second, low_column)
    return next_start[None], nodes[None]


def solution(mesh):
    in_specs = (P("tm", None, "space", None), P("tm", None, None, "space", None))
    out_specs = (P("tm", None, "space", None), P("tm", None, None, "space", None))
    return jax.shard_map(body, mesh=mesh, in_specs=in_specs, out_specs=out_specs, check_vma=False)
```

```python
import functools

import jax
import jax.numpy as jnp
from jax import lax
from jax.experimental import pallas as pl
from jax.experimental.pallas import tpu as pltpu
from jax.sharding import PartitionSpec as P


COARSE_SHARE = 4
LANES = 128
STRIP = 32
HALO = 4
PAD = 8

diffusion = 1.5
drift = 0.8
shear = 0.6


def rates(row_start, rows, column_start, columns, size_x, size_y):
    row = row_start + lax.broadcasted_iota(jnp.int32, (rows, columns), 0)
    column = column_start + lax.broadcasted_iota(jnp.int32, (rows, columns), 1)
    along = (row.astype(jnp.float32) - size_x // 2) * (2.0 / size_x)
    across = (column.astype(jnp.float32) - size_y // 2) * (2.0 / size_y)
    real = -diffusion * (along * along + across * across)
    return real, -drift * across, shear * across


def turned(real, imag, first, second):
    return real * first - imag * second, real * second + imag * first


def fine_kernel(*refs, first_block, coarse, size_x, size_y, coarse_rows, pieces, aliased):
    begin_hbm, old_hbm = refs[:2]
    refs = refs[2:]
    if coarse:
        before, after = refs[:2]
        refs = refs[2:]
    refs = refs[aliased:]
    nodes, refs = refs[0], refs[1:]
    sends, refs = refs[: len(pieces)], refs[len(pieces):]
    offset = None
    if coarse:
        offset, refs = refs[0], refs[1:]
    wide_one, wide_two, inner, inverse, begin_all, old_all, sems = refs
    rows = begin_hbm.shape[1]
    step = pl.program_id(0)

    def loads(k):
        cut = pl.ds((first_block + k) * LANES, LANES)
        return (pltpu.make_async_copy(begin_hbm.at[:, :, cut], begin_all.at[k], sems.at[0, k]),
                pltpu.make_async_copy(old_hbm.at[:, :, :, cut], old_all.at[k], sems.at[1, k]))

    @pl.when(step == 0)
    def _():
        for k in range(begin_all.shape[0]):
            for copy in loads(k):
                copy.start()

    for copy in loads(step):
        copy.wait()
    begin = begin_all.at[step]
    old = old_all.at[step]
    rank = lax.axis_index("space")
    ranks = lax.axis_size("space")
    spot = pl.ds(pl.multiple_of(pl.program_id(0) * LANES, LANES), LANES)
    row_base = rank * rows
    column_base = (first_block + pl.program_id(0)) * LANES
    has_before = rank > 0
    has_after = rank < ranks - 1
    tiles = [("in", start, min(STRIP, rows - start)) for start in range(0, rows, STRIP)]
    if coarse:
        whole = pl.ds((first_block + pl.program_id(0)) * LANES, LANES)
        tiles = [("before", -HALO, HALO)] + tiles + [("after", rows, HALO)]

    def fields(kind, start, count):
        if kind == "in":
            here = pl.ds(start, count)
            return ([begin[0, here, :], begin[1, here, :]],
                    [old[0, 0, here, :], old[0, 1, here, :]],
                    [old[1, 0, here, :], old[1, 1, here, :]])
        side = before if kind == "before" else after
        part = [side[k, :, whole] for k in range(6)]
        return (part[:2], part[2:4], part[4:])

    def kept(kind, value):
        if kind == "before":
            return jnp.where(has_before, value, 0.0)
        if kind == "after":
            return jnp.where(has_after, value, 0.0)
        return value

    def sums(ref, part, start, count):
        return ref[part, pl.ds(PAD + start - 1, count), :] + ref[part, pl.ds(PAD + start + 1, count), :]

    for kind, start, count in tiles:
        b, one, two = fields(kind, start, count)
        for part in range(2):
            third = (1.0 / 3.0) * one[part]
            wide_one[part, pl.ds(PAD + start, count), :] = (5.0 / 24.0) * b[part] + third - (1.0 / 24.0) * two[part]
            wide_two[part, pl.ds(PAD + start, count), :] = third - (1.0 / 24.0) * b[part] + (5.0 / 24.0) * two[part] - 0.5 * one[part]
    for kind, start, count in tiles:
        real, imag, factor = rates(row_base + start, count, column_base, LANES, size_x, size_y)
        b, one, _ = fields(kind, start, count)
        here = pl.ds(PAD + start, count)
        u = [wide_one[part, here, :] - 0.5 * one[part] for part in range(2)]
        lu = turned(real, imag, u[0], u[1])
        top = (b[0] + lu[0] + factor * sums(wide_one, 1, start, count),
               b[1] + lu[1] - factor * sums(wide_one, 0, start, count))
        half_real = 1.0 - 0.5 * real
        half_imag = -0.5 * imag
        share = 1.0 / (half_real * half_real + half_imag * half_imag)
        half_real = half_real * share
        half_imag = half_imag * share
        inverse[0, here, :] = half_real
        inverse[1, here, :] = half_imag
        node = (top[0] * half_real + top[1] * half_imag, top[1] * half_real - top[0] * half_imag)
        for part in range(2):
            value = kept(kind, node[part])
            if kind == "in":
                nodes[0, part, pl.ds(start, count), :] = value
            inner[part, here, :] = value
    for kind, start, count in tiles:
        here = pl.ds(PAD + start, count)
        for part in range(2):
            wide_one[part, here, :] = 0.5 * inner[part, here, :] + wide_two[part, here, :]
    for kind, start, count in tiles:
        if kind != "in" and not coarse:
            continue
        real, imag, factor = rates(row_base + start, count, column_base, LANES, size_x, size_y)
        b, one, two = fields(kind, start, count)
        here = pl.ds(PAD + start, count)
        u = [wide_two[part, here, :] + 0.5 * (one[part] - two[part]) for part in range(2)]
        lu = turned(real, imag, u[0], u[1])
        n1 = [inner[part, here, :] for part in range(2)]
        top = (n1[0] + lu[0] + factor * sums(wide_one, 1, start, count),
               n1[1] + lu[1] - factor * sums(wide_one, 0, start, count))
        half_real = inverse[0, here, :]
        half_imag = inverse[1, here, :]
        node = (top[0] * half_real + top[1] * half_imag, top[1] * half_real - top[0] * half_imag)
        for part in range(2):
            value = kept(kind, node[part])
            if kind == "in":
                nodes[1, part, pl.ds(start, count), :] = value
                for (low, high), send in zip(pieces, sends):
                    a, z = max(low, start), min(high, start + count)
                    if a < z:
                        send[part, pl.ds(a - low, z - a), spot] = value[a - start:z - start]
            if coarse:
                inner[part, here, :] = (1.0 / 6.0) * b[part] + (2.0 / 3.0) * n1[part] + (1.0 / 6.0) * value
    if coarse:
        def offsets(shift):
            for start in range(0, coarse_rows, STRIP):
                count = min(STRIP, coarse_rows - start)
                at = shift + start
                real, imag, factor = rates(row_base + at, count, column_base, LANES, size_x, size_y)
                v = [inner[part, pl.ds(PAD + at, count), :] for part in range(2)]
                e = [nodes[1, part, pl.ds(at, count), :] for part in range(2)]
                lu = turned(real, imag, v[0] - e[0], v[1] - e[1])
                off = (lu[0] + factor * sums(inner, 1, at, count),
                       lu[1] - factor * sums(inner, 0, at, count))
                step_real = 1.0 - real
                step_imag = -imag
                share = 1.0 / (step_real * step_real + step_imag * step_imag)
                lead = lax.axis_index("tm") == 0
                off = tuple(off[part] + jnp.where(lead, begin[part, pl.ds(at, count), :], 0.0) for part in range(2))
                offset[0, pl.ds(start, count), spot] = (off[0] * step_real + off[1] * step_imag) * share
                offset[1, pl.ds(start, count), spot] = (off[1] * step_real - off[0] * step_imag) * share

        low_shift = rows - coarse_rows
        if low_shift == 0:
            offsets(0)
        else:
            upper = rank >= ranks // 2

            @pl.when(upper)
            def _():
                offsets(0)

            @pl.when(jnp.logical_not(upper))
            def _():
                offsets(low_shift)


VMEM = pl.BlockSpec(memory_space=pltpu.VMEM)
ANY = pl.BlockSpec(memory_space=pl.ANY)
HBM = pl.BlockSpec(memory_space=pltpu.HBM)


def grant(mebibytes):
    return pltpu.CompilerParams(vmem_limit_bytes=mebibytes * 1024 * 1024)


PARAMS = grant(28)


def fine_call(begin, old, halo, nodes, first, width, pieces, size_x, coarse_rows, params):
    rows, columns = begin.shape[1:]
    coarse = halo is not None
    base = first // LANES
    f32 = jnp.float32
    out_shape = [jax.ShapeDtypeStruct((2, 2, rows, columns), f32)]
    out_specs = [pl.BlockSpec((2, 2, rows, LANES), lambda j: (0, 0, 0, base + j))]
    for low, high in pieces:
        out_shape.append(jax.ShapeDtypeStruct((2, high - low, width), f32))
        out_specs.append(VMEM)
    if coarse:
        out_shape.append(jax.ShapeDtypeStruct((2, coarse_rows, width), f32))
        out_specs.append(VMEM)
    in_specs = [HBM, HBM]
    operands = [begin, old]
    if coarse:
        operands += list(halo)
        in_specs += [VMEM, VMEM]
    aliases = {}
    if nodes is not None:
        aliases = {len(operands): 0}
        operands.append(nodes)
        in_specs.append(ANY)
    kernel = functools.partial(
        fine_kernel, first_block=base, coarse=coarse, size_x=size_x, size_y=columns,
        coarse_rows=coarse_rows, pieces=pieces, aliased=len(aliases))
    blocks = width // LANES
    scratch = [pltpu.VMEM((2, rows + 2 * PAD, LANES), f32) for _ in range(4)]
    scratch += [pltpu.VMEM((blocks, 2, rows, LANES), f32), pltpu.VMEM((blocks, 2, 2, rows, LANES), f32),
                pltpu.SemaphoreType.DMA((2, blocks))]
    return pl.pallas_call(
        kernel, grid=(blocks,), in_specs=in_specs, out_specs=out_specs, out_shape=out_shape,
        scratch_shapes=scratch, input_output_aliases=aliases, compiler_params=params,
        name="fine_coarse" if coarse else "fine",
    )(*operands)


def edge_kernel(begin_hbm, old_hbm, before, after, _, nodes, send, wide, fixed, begin_sides, old_sides, sems,
                *, rows, size_x, size_y, outer):
    rank = lax.axis_index("space")
    side_rows = begin_sides.shape[2]
    height = HALO + side_rows
    loads = []
    for k in range(2):
        cut = pl.ds(0 if k == 0 else rows - side_rows, side_rows)
        loads.append(pltpu.make_async_copy(begin_hbm.at[:, cut, :], begin_sides.at[k], sems.at[k]))
        loads.append(pltpu.make_async_copy(old_hbm.at[:, :, cut, :], old_sides.at[k], sems.at[2 + k]))
    for copy in loads:
        copy.start()
    for copy in loads:
        copy.wait()
    begin_top, begin_end = begin_sides.at[0], begin_sides.at[1]
    old_top, old_end = old_sides.at[0], old_sides.at[1]
    copies = []
    for k, (low, width, spot) in enumerate(outer):
        cut = pl.ds(low, width)
        for top in (True, False):
            begin, old, halo = (begin_top, old_top, before) if top else (begin_end, old_end, after)
            base = rank * rows + (-HALO if top else rows - side_rows)

            def field(index):
                if index < 2:
                    near = begin[index, :, cut]
                else:
                    near = old[index // 2 - 1, index % 2, :, cut]
                far = halo[index, :, cut]
                return jnp.concatenate([far, near] if top else [near, far], axis=0)

            real, imag, factor = rates(base, height, low, width, size_x, size_y)
            b, one, two = [[field(2 * k + part) for part in range(2)] for k in range(3)]

            def coupled(pair):
                moved = []
                for part in range(2):
                    wide[part, pl.ds(PAD, height), :] = pair[part]
                    moved.append(wide[part, pl.ds(PAD - 1, height), :] + wide[part, pl.ds(PAD + 1, height), :])
                return factor * moved[1], -factor * moved[0]

            half_real = 1.0 - 0.5 * real
            half_imag = -0.5 * imag
            share = 1.0 / (half_real * half_real + half_imag * half_imag)

            def divided(x, y):
                return (x * half_real + y * half_imag) * share, (y * half_real - x * half_imag) * share

            w1 = [(5.0 / 24.0) * b[p] + (1.0 / 3.0) * one[p] - (1.0 / 24.0) * two[p] for p in range(2)]
            w2 = [(1.0 / 3.0) * one[p] - (1.0 / 24.0) * b[p] + (5.0 / 24.0) * two[p] for p in range(2)]
            lu = turned(real, imag, w1[0] - 0.5 * one[0], w1[1] - 0.5 * one[1])
            cw = coupled(w1)
            n1 = divided(b[0] + lu[0] + cw[0], b[1] + lu[1] + cw[1])
            row = base + lax.broadcasted_iota(jnp.int32, (height, width), 0)
            inside = jnp.logical_and(row >= 0, row < size_x)
            n1 = [jnp.where(inside, value, 0.0) for value in n1]
            cw = coupled([0.5 * (n1[p] - one[p]) + w2[p] for p in range(2)])
            lu = turned(real, imag, w2[0] - 0.5 * two[0], w2[1] - 0.5 * two[1])
            n2 = divided(n1[0] + lu[0] + cw[0], n1[1] + lu[1] + cw[1])
            keep = slice(HALO, HALO + PAD) if top else slice(side_rows - PAD, side_rows)
            at = 0 if top else PAD
            for part in range(2):
                fixed[0, part, pl.ds(at, PAD), pl.ds(spot, width)] = n1[part][keep]
                fixed[1, part, pl.ds(at, PAD), pl.ds(spot, width)] = n2[part][keep]
                send[part, pl.ds(at, PAD), pl.ds(spot, width)] = n2[part][keep]
            copy = pltpu.make_async_copy(
                fixed.at[:, :, pl.ds(at, PAD), pl.ds(spot, width)],
                nodes.at[:, :, pl.ds(0 if top else rows - PAD, PAD), cut], sems.at[4 + 2 * k + (not top)])
            copy.start()
            copies.append(copy)
    for copy in copies:
        copy.wait()


def edge_call(begin, old, halo, nodes, outer, size_x):
    rows, columns = begin.shape[1:]
    side = 2 * PAD
    total = sum(width for _, width in outer)
    f32 = jnp.float32
    spots, at = [], 0
    for low, width in outer:
        spots.append((low, width, at))
        at += width
    widest = max(width for _, width in outer)
    assert all(width == widest for _, width in outer)
    kernel = functools.partial(edge_kernel, rows=rows, size_x=size_x, size_y=columns, outer=spots)
    return pl.pallas_call(
        kernel, grid=(1,),
        in_specs=[HBM, HBM, VMEM, VMEM, ANY],
        out_specs=[ANY, VMEM],
        out_shape=[jax.ShapeDtypeStruct(nodes.shape, f32), jax.ShapeDtypeStruct((2, side, total), f32)],
        scratch_shapes=[pltpu.VMEM((2, 2 * PAD + HALO + side + PAD, widest), f32),
                        pltpu.VMEM((2, 2, side, total), f32), pltpu.VMEM((2, 2, side, columns), f32),
                        pltpu.VMEM((2, 2, 2, side, columns), f32), pltpu.SemaphoreType.DMA((4 + 2 * len(outer),))],
        input_output_aliases={4: 0}, compiler_params=grant(57), name="edges",
    )(begin, old, halo[0], halo[1], nodes)


def patch_kernel(*refs, count, pieces, coarse_rows):
    begin, nodes_in = refs[:2]
    arrived = refs[2:2 + count]
    fresh, finish, start, nodes = refs[2 + count:]
    rows = begin.shape[1]
    rank = lax.axis_index("space")
    ranks = lax.axis_size("space")
    lead = lax.axis_index("tm") == 0
    spot = pl.ds(pl.multiple_of(pl.program_id(0) * LANES, LANES), LANES)
    middle = jnp.logical_or(rank == ranks // 2, rank == ranks // 2 - 1)
    for (low, high), piece in zip(pieces, arrived):
        here = pl.ds(low, high - low)
        for part in range(2):
            start[part, here, :] = jnp.where(lead, begin[part, here, :], piece[part, :, spot])
    nodes[...] = nodes_in[...]

    def fix(shift):
        here = pl.ds(shift, coarse_rows)
        for part in range(2):
            old_begin = begin[part, here, :]
            n2 = nodes_in[1, part, here, :]
            now = jnp.where(lead, old_begin, fresh[part, :, spot])
            change = finish[part, :, spot] - n2
            nodes[0, part, here, :] = nodes_in[0, part, here, :] + 0.5 * ((now - old_begin) + change)
            nodes[1, part, here, :] = n2 + change
            start[part, here, :] = now

    if rows == coarse_rows:
        @pl.when(middle)
        def _():
            fix(0)
    else:
        @pl.when(rank == ranks // 2)
        def _():
            fix(0)

        @pl.when(rank == ranks // 2 - 1)
        def _():
            fix(rows - coarse_rows)


def patch_call(begin, nodes, arrived, pieces, fresh, finish, low_column, coarse_rows):
    rows = begin.shape[1]
    base = low_column // LANES
    begin_spec = pl.BlockSpec((2, rows, LANES), lambda j: (0, 0, base + j))
    nodes_spec = pl.BlockSpec((2, 2, rows, LANES), lambda j: (0, 0, 0, base + j))
    kernel = functools.partial(patch_kernel, count=len(arrived), pieces=pieces, coarse_rows=coarse_rows)
    return pl.pallas_call(
        kernel, grid=(fresh.shape[2] // LANES,),
        in_specs=[begin_spec, nodes_spec] + [VMEM] * (len(arrived) + 2),
        out_specs=[begin_spec, nodes_spec],
        out_shape=[jax.ShapeDtypeStruct(begin.shape, jnp.float32), jax.ShapeDtypeStruct(nodes.shape, jnp.float32)],
        input_output_aliases={1: 1}, compiler_params=PARAMS, name="patch",
    )(begin, nodes, *arrived, fresh, finish)


def place_kernel(begin, middle, edges, _, start, *, spot):
    lead = lax.axis_index("tm") == 0
    rows = begin.shape[1]
    here = pl.ds(pl.multiple_of(pl.program_id(0) * LANES, LANES), LANES)
    side = pl.ds(pl.multiple_of(spot + pl.program_id(0) * LANES, LANES), LANES)
    for part in range(2):
        start[part, pl.ds(0, PAD), :] = jnp.where(lead, begin[part, pl.ds(0, PAD), :], edges[part, pl.ds(0, PAD), side])
        start[part, pl.ds(PAD, rows - 2 * PAD), :] = jnp.where(
            lead, begin[part, pl.ds(PAD, rows - 2 * PAD), :], middle[part, :, here])
        start[part, pl.ds(rows - PAD, PAD), :] = jnp.where(
            lead, begin[part, pl.ds(rows - PAD, PAD), :], edges[part, pl.ds(PAD, PAD), side])


def place_call(begin, middle, edges, start, first, spot):
    rows = begin.shape[1]
    base = first // LANES
    spec = pl.BlockSpec((2, rows, LANES), lambda j: (0, 0, base + j))
    return pl.pallas_call(
        functools.partial(place_kernel, spot=spot), grid=(middle.shape[2] // LANES,),
        in_specs=[spec, VMEM, VMEM, ANY], out_specs=spec,
        out_shape=jax.ShapeDtypeStruct(begin.shape, jnp.float32),
        input_output_aliases={3: 0}, compiler_params=PARAMS, name="place",
    )(begin, middle, edges, start)


def powers(row_base, rows, low_column, width, size_x, size_y):
    real, imag, _ = rates(row_base, rows, low_column, width, size_x, size_y)
    step_real = 1.0 - real
    step_imag = -imag
    share = 1.0 / (step_real * step_real + step_imag * step_imag)
    return step_real * share, -step_imag * share


def body(start_values, node_values):
    begin = start_values[0]
    old = node_values[0]
    rows, columns = begin.shape[1:]
    slices, ranks = lax.axis_size("tm"), lax.axis_size("space")
    size_x = rows * ranks
    width = columns // COARSE_SHARE
    low_column = columns // 2 - width // 2
    coarse_rows = min(rows, size_x // COARSE_SHARE // 2)
    lower, upper = ranks // 2 - 1, ranks // 2
    rank = lax.axis_index("space")
    lead = lax.axis_index("tm") == 0

    def edge(low):
        cut = [begin[:, low:low + HALO], old[0, :, low:low + HALO], old[1, :, low:low + HALO]]
        return jnp.concatenate(cut, axis=0)

    up = [(i, i + 1) for i in range(ranks - 1)]
    before = lax.ppermute(edge(rows - HALO), "space", up)
    after = lax.ppermute(edge(0), "space", [(j, i) for i, j in up])

    def ahead(value, steps, members):
        pairs = [(n * ranks + s, (n + steps) * ranks + s) for n in range(slices - steps) for s in members]
        return lax.ppermute(value, ("tm", "space"), pairs)

    everyone = range(ranks)
    middle = (lower, upper)
    if rows == coarse_rows:
        pieces = [(0, rows)]
        holders = [[s for s in everyone if s not in middle]]
    else:
        cuts = [0, coarse_rows, rows - coarse_rows, rows]
        pieces = [(a, b) for a, b in zip(cuts, cuts[1:]) if a < b]
        holders = [[s for s in everyone
                    if not (s == upper and b <= coarse_rows) and not (s == lower and a >= rows - coarse_rows)]
                   for a, b in pieces]
    second = low_column + width
    rest = columns - second
    inside = [(PAD, rows - PAD)]
    nodes, left = fine_call(begin, old, None, None, 0, low_column, inside, size_x, coarse_rows, grant(62))
    left = ahead(left, 1, everyone)
    made = fine_call(begin, old, (before, after), nodes, low_column, width, pieces, size_x, coarse_rows, grant(60))
    nodes, inner_sends, offset = made[0], made[1:-1], made[-1]
    one_back = ahead(offset, 1, middle)
    two_back = ahead(offset, 2, middle)
    nodes, right = fine_call(begin, old, None, nodes, second, rest, inside, size_x, coarse_rows, grant(58))
    right = ahead(right, 1, everyone)
    nodes, edges = edge_call(begin, old, (before, after), nodes, [(0, low_column), (second, rest)], size_x)
    edges = ahead(edges, 1, everyone)

    shift = jnp.where(rank >= ranks // 2, 0, rows - coarse_rows)
    d_real, d_imag = powers(rank * rows + shift, coarse_rows, low_column, width, size_x, columns)

    def add(total, field, real, imag):
        grown = turned(real, imag, field[0], field[1])
        return jnp.stack([total[0] + grown[0], total[1] + grown[1]])

    total = add(one_back, two_back, d_real, d_imag)
    inner = [ahead(piece, 1, members) for piece, members in zip(inner_sends, holders)]
    power = turned(d_real, d_imag, d_real, d_imag)
    reach = 2
    while reach < slices:
        total = add(total, ahead(total, reach, middle), *power)
        power = turned(power[0], power[1], power[0], power[1])
        reach *= 2
    end = add(offset, jnp.where(lead, 0.0, total), d_real, d_imag)
    next_start, nodes = patch_call(begin, nodes, inner, pieces, total, end, low_column, coarse_rows)
    next_start = place_call(begin, left, edges, next_start, 0, 0)
    next_start = place_call(begin, right, edges, next_start, second, low_column)
    return next_start[None], nodes[None]


def solution(mesh):
    in_specs = (P("tm", None, "space", None), P("tm", None, None, "space", None))
    out_specs = (P("tm", None, "space", None), P("tm", None, None, "space", None))
    return jax.shard_map(body, mesh=mesh, in_specs=in_specs, out_specs=out_specs, check_vma=False)
```

```python
import functools

import jax
import jax.numpy as jnp
from jax import lax
from jax.experimental import pallas as pl
from jax.experimental.pallas import tpu as pltpu
from jax.sharding import PartitionSpec as P


COARSE_SHARE = 4
LANES = 128
STRIP = 32
HALO = 4
PAD = 8


diffusion = 1.5
drift = 0.8
shear = 0.6


def rates(row_start, rows, column_start, columns, size_x, size_y):
    row = row_start + lax.broadcasted_iota(jnp.int32, (rows, columns), 0)
    column = column_start + lax.broadcasted_iota(jnp.int32, (rows, columns), 1)
    along = (row.astype(jnp.float32) - size_x // 2) * (2.0 / size_x)
    across = (column.astype(jnp.float32) - size_y // 2) * (2.0 / size_y)
    real = -diffusion * (along * along + across * across)
    return real, -drift * across, shear * across


def turned(real, imag, first, second):
    return real * first - imag * second, real * second + imag * first


def fine_kernel(*refs, first_block, coarse, size_x, size_y, coarse_rows, pieces, aliased):
    begin_hbm, old_hbm = refs[:2]
    refs = refs[2:]
    if coarse:
        before, after = refs[:2]
        refs = refs[2:]
    refs = refs[aliased:]
    nodes, refs = refs[0], refs[1:]
    sends, refs = refs[: len(pieces)], refs[len(pieces):]
    offset = None
    if coarse:
        offset, refs = refs[0], refs[1:]
    wide_one, wide_two, inner, inverse, begin_all, old_all, sems = refs
    rows = begin_hbm.shape[1]
    step = pl.program_id(0)

    def loads(k):
        cut = pl.ds((first_block + k) * LANES, LANES)
        return (pltpu.make_async_copy(begin_hbm.at[:, :, cut], begin_all.at[k], sems.at[0, k]),
                pltpu.make_async_copy(old_hbm.at[:, :, :, cut], old_all.at[k], sems.at[1, k]))

    @pl.when(step == 0)
    def _():
        for k in range(begin_all.shape[0]):
            for copy in loads(k):
                copy.start()

    for copy in loads(step):
        copy.wait()
    begin = begin_all.at[step]
    old = old_all.at[step]
    rank = lax.axis_index("space")
    ranks = lax.axis_size("space")
    spot = pl.ds(pl.multiple_of(pl.program_id(0) * LANES, LANES), LANES)
    row_base = rank * rows
    column_base = (first_block + pl.program_id(0)) * LANES
    has_before = rank > 0
    has_after = rank < ranks - 1
    tiles = [("in", start, min(STRIP, rows - start)) for start in range(0, rows, STRIP)]
    if coarse:
        whole = pl.ds((first_block + pl.program_id(0)) * LANES, LANES)
        tiles = [("before", -HALO, HALO)] + tiles + [("after", rows, HALO)]

    def fields(kind, start, count):
        if kind == "in":
            here = pl.ds(start, count)
            return ([begin[0, here, :], begin[1, here, :]],
                    [old[0, 0, here, :], old[0, 1, here, :]],
                    [old[1, 0, here, :], old[1, 1, here, :]])
        side = before if kind == "before" else after
        part = [side[k, :, whole] for k in range(6)]
        return (part[:2], part[2:4], part[4:])

    def kept(kind, value):
        if kind == "before":
            return jnp.where(has_before, value, 0.0)
        if kind == "after":
            return jnp.where(has_after, value, 0.0)
        return value

    def sums(ref, part, start, count):
        return ref[part, pl.ds(PAD + start - 1, count), :] + ref[part, pl.ds(PAD + start + 1, count), :]

    for kind, start, count in tiles:
        b, one, two = fields(kind, start, count)
        for part in range(2):
            third = (1.0 / 3.0) * one[part]
            wide_one[part, pl.ds(PAD + start, count), :] = (5.0 / 24.0) * b[part] + third - (1.0 / 24.0) * two[part]
            wide_two[part, pl.ds(PAD + start, count), :] = third - (1.0 / 24.0) * b[part] + (5.0 / 24.0) * two[part] - 0.5 * one[part]
    for kind, start, count in tiles:
        real, imag, factor = rates(row_base + start, count, column_base, LANES, size_x, size_y)
        b, one, _ = fields(kind, start, count)
        here = pl.ds(PAD + start, count)
        u = [wide_one[part, here, :] - 0.5 * one[part] for part in range(2)]
        lu = turned(real, imag, u[0], u[1])
        top = (b[0] + lu[0] + factor * sums(wide_one, 1, start, count),
               b[1] + lu[1] - factor * sums(wide_one, 0, start, count))
        half_real = 1.0 - 0.5 * real
        half_imag = -0.5 * imag
        share = 1.0 / (half_real * half_real + half_imag * half_imag)
        half_real = half_real * share
        half_imag = half_imag * share
        inverse[0, here, :] = half_real
        inverse[1, here, :] = half_imag
        node = (top[0] * half_real + top[1] * half_imag, top[1] * half_real - top[0] * half_imag)
        for part in range(2):
            value = kept(kind, node[part])
            if kind == "in":
                nodes[0, part, pl.ds(start, count), :] = value
            inner[part, here, :] = value
    for kind, start, count in tiles:
        here = pl.ds(PAD + start, count)
        for part in range(2):
            wide_one[part, here, :] = 0.5 * inner[part, here, :] + wide_two[part, here, :]
    for kind, start, count in tiles:
        if kind != "in" and not coarse:
            continue
        real, imag, factor = rates(row_base + start, count, column_base, LANES, size_x, size_y)
        b, one, two = fields(kind, start, count)
        here = pl.ds(PAD + start, count)
        u = [wide_two[part, here, :] + 0.5 * (one[part] - two[part]) for part in range(2)]
        lu = turned(real, imag, u[0], u[1])
        n1 = [inner[part, here, :] for part in range(2)]
        top = (n1[0] + lu[0] + factor * sums(wide_one, 1, start, count),
               n1[1] + lu[1] - factor * sums(wide_one, 0, start, count))
        half_real = inverse[0, here, :]
        half_imag = inverse[1, here, :]
        node = (top[0] * half_real + top[1] * half_imag, top[1] * half_real - top[0] * half_imag)
        for part in range(2):
            value = kept(kind, node[part])
            if kind == "in":
                nodes[1, part, pl.ds(start, count), :] = value
                for (low, high), send in zip(pieces, sends):
                    if high - low == rows - coarse_rows and coarse:
                        continue
                    a, z = max(low, start), min(high, start + count)
                    if a < z:
                        send[part, pl.ds(a - low, z - a), spot] = value[a - start:z - start]
            if coarse:
                inner[part, here, :] = (1.0 / 6.0) * b[part] + (2.0 / 3.0) * n1[part] + (1.0 / 6.0) * value
    if coarse:
        def offsets(shift):
            for start in range(0, coarse_rows, STRIP):
                count = min(STRIP, coarse_rows - start)
                at = shift + start
                real, imag, factor = rates(row_base + at, count, column_base, LANES, size_x, size_y)
                v = [inner[part, pl.ds(PAD + at, count), :] for part in range(2)]
                e = [nodes[1, part, pl.ds(at, count), :] for part in range(2)]
                lu = turned(real, imag, v[0] - e[0], v[1] - e[1])
                off = (lu[0] + factor * sums(inner, 1, at, count),
                       lu[1] - factor * sums(inner, 0, at, count))
                step_real = 1.0 - real
                step_imag = -imag
                share = 1.0 / (step_real * step_real + step_imag * step_imag)
                lead = lax.axis_index("tm") == 0
                off = tuple(off[part] + jnp.where(lead, begin[part, pl.ds(at, count), :], 0.0) for part in range(2))
                offset[0, pl.ds(start, count), spot] = (off[0] * step_real + off[1] * step_imag) * share
                offset[1, pl.ds(start, count), spot] = (off[1] * step_real - off[0] * step_imag) * share
            if rows > coarse_rows:
                from_row = 0 if shift else coarse_rows
                for part in range(2):
                    sends[1][part, :, spot] = nodes[1, part, pl.ds(from_row, rows - coarse_rows), :]

        low_shift = rows - coarse_rows
        if low_shift == 0:
            offsets(0)
        else:
            upper = rank >= ranks // 2

            @pl.when(upper)
            def _():
                offsets(0)

            @pl.when(jnp.logical_not(upper))
            def _():
                offsets(low_shift)


VMEM = pl.BlockSpec(memory_space=pltpu.VMEM)
ANY = pl.BlockSpec(memory_space=pl.ANY)
HBM = pl.BlockSpec(memory_space=pltpu.HBM)


def grant(mebibytes):
    return pltpu.CompilerParams(vmem_limit_bytes=mebibytes * 1024 * 1024)


PARAMS = grant(28)


def fine_call(begin, old, halo, nodes, first, width, pieces, size_x, coarse_rows, params):
    rows, columns = begin.shape[1:]
    coarse = halo is not None
    base = first // LANES
    f32 = jnp.float32
    out_shape = [jax.ShapeDtypeStruct((2, 2, rows, columns), f32)]
    out_specs = [pl.BlockSpec((2, 2, rows, LANES), lambda j: (0, 0, 0, base + j))]
    for low, high in pieces:
        out_shape.append(jax.ShapeDtypeStruct((2, high - low, width), f32))
        out_specs.append(VMEM)
    if coarse:
        out_shape.append(jax.ShapeDtypeStruct((2, coarse_rows, width), f32))
        out_specs.append(VMEM)
    in_specs = [HBM, HBM]
    operands = [begin, old]
    if coarse:
        operands += list(halo)
        in_specs += [VMEM, VMEM]
    aliases = {}
    if nodes is not None:
        aliases = {len(operands): 0}
        operands.append(nodes)
        in_specs.append(ANY)
    kernel = functools.partial(
        fine_kernel, first_block=base, coarse=coarse, size_x=size_x, size_y=columns,
        coarse_rows=coarse_rows, pieces=pieces, aliased=len(aliases))
    blocks = width // LANES
    scratch = [pltpu.VMEM((2, rows + 2 * PAD, LANES), f32) for _ in range(4)]
    scratch += [pltpu.VMEM((blocks, 2, rows, LANES), f32), pltpu.VMEM((blocks, 2, 2, rows, LANES), f32),
                pltpu.SemaphoreType.DMA((2, blocks))]
    return pl.pallas_call(
        kernel, grid=(blocks,), in_specs=in_specs, out_specs=out_specs, out_shape=out_shape,
        scratch_shapes=scratch, input_output_aliases=aliases, compiler_params=params,
        name="fine_coarse" if coarse else "fine",
    )(*operands)


def edge_kernel(begin_hbm, old_hbm, before, after, _, nodes, send, wide, fixed, begin_sides, old_sides, sems,
                *, rows, size_x, size_y, outer):
    rank = lax.axis_index("space")
    side_rows = begin_sides.shape[2]
    height = HALO + side_rows
    loads = []
    for k in range(2):
        cut = pl.ds(0 if k == 0 else rows - side_rows, side_rows)
        loads.append(pltpu.make_async_copy(begin_hbm.at[:, cut, :], begin_sides.at[k], sems.at[k]))
        loads.append(pltpu.make_async_copy(old_hbm.at[:, :, cut, :], old_sides.at[k], sems.at[2 + k]))
    for copy in loads:
        copy.start()
    for copy in loads:
        copy.wait()
    begin_top, begin_end = begin_sides.at[0], begin_sides.at[1]
    old_top, old_end = old_sides.at[0], old_sides.at[1]
    copies = []
    for k, (low, width, spot) in enumerate(outer):
        cut = pl.ds(low, width)
        for top in (True, False):
            begin, old, halo = (begin_top, old_top, before) if top else (begin_end, old_end, after)
            base = rank * rows + (-HALO if top else rows - side_rows)

            def field(index):
                if index < 2:
                    near = begin[index, :, cut]
                else:
                    near = old[index // 2 - 1, index % 2, :, cut]
                far = halo[index, :, cut]
                return jnp.concatenate([far, near] if top else [near, far], axis=0)

            real, imag, factor = rates(base, height, low, width, size_x, size_y)
            b, one, two = [[field(2 * k + part) for part in range(2)] for k in range(3)]

            def coupled(pair):
                moved = []
                for part in range(2):
                    wide[part, pl.ds(PAD, height), :] = pair[part]
                    moved.append(wide[part, pl.ds(PAD - 1, height), :] + wide[part, pl.ds(PAD + 1, height), :])
                return factor * moved[1], -factor * moved[0]

            half_real = 1.0 - 0.5 * real
            half_imag = -0.5 * imag
            share = 1.0 / (half_real * half_real + half_imag * half_imag)

            def divided(x, y):
                return (x * half_real + y * half_imag) * share, (y * half_real - x * half_imag) * share

            w1 = [(5.0 / 24.0) * b[p] + (1.0 / 3.0) * one[p] - (1.0 / 24.0) * two[p] for p in range(2)]
            w2 = [(1.0 / 3.0) * one[p] - (1.0 / 24.0) * b[p] + (5.0 / 24.0) * two[p] for p in range(2)]
            lu = turned(real, imag, w1[0] - 0.5 * one[0], w1[1] - 0.5 * one[1])
            cw = coupled(w1)
            n1 = divided(b[0] + lu[0] + cw[0], b[1] + lu[1] + cw[1])
            row = base + lax.broadcasted_iota(jnp.int32, (height, width), 0)
            inside = jnp.logical_and(row >= 0, row < size_x)
            n1 = [jnp.where(inside, value, 0.0) for value in n1]
            cw = coupled([0.5 * (n1[p] - one[p]) + w2[p] for p in range(2)])
            lu = turned(real, imag, w2[0] - 0.5 * two[0], w2[1] - 0.5 * two[1])
            n2 = divided(n1[0] + lu[0] + cw[0], n1[1] + lu[1] + cw[1])
            keep = slice(HALO, HALO + PAD) if top else slice(side_rows - PAD, side_rows)
            at = 0 if top else PAD
            for part in range(2):
                fixed[0, part, pl.ds(at, PAD), pl.ds(spot, width)] = n1[part][keep]
                fixed[1, part, pl.ds(at, PAD), pl.ds(spot, width)] = n2[part][keep]
                send[part, pl.ds(at, PAD), pl.ds(spot, width)] = n2[part][keep]
            copy = pltpu.make_async_copy(
                fixed.at[:, :, pl.ds(at, PAD), pl.ds(spot, width)],
                nodes.at[:, :, pl.ds(0 if top else rows - PAD, PAD), cut], sems.at[4 + 2 * k + (not top)])
            copy.start()
            copies.append(copy)
    for copy in copies:
        copy.wait()


def edge_call(begin, old, halo, nodes, outer, size_x):
    rows, columns = begin.shape[1:]
    side = 2 * PAD
    total = sum(width for _, width in outer)
    f32 = jnp.float32
    spots, at = [], 0
    for low, width in outer:
        spots.append((low, width, at))
        at += width
    widest = max(width for _, width in outer)
    assert all(width == widest for _, width in outer)
    kernel = functools.partial(edge_kernel, rows=rows, size_x=size_x, size_y=columns, outer=spots)
    return pl.pallas_call(
        kernel, grid=(1,),
        in_specs=[HBM, HBM, VMEM, VMEM, ANY],
        out_specs=[ANY, VMEM],
        out_shape=[jax.ShapeDtypeStruct(nodes.shape, f32), jax.ShapeDtypeStruct((2, side, total), f32)],
        scratch_shapes=[pltpu.VMEM((2, 2 * PAD + HALO + side + PAD, widest), f32),
                        pltpu.VMEM((2, 2, side, total), f32), pltpu.VMEM((2, 2, side, columns), f32),
                        pltpu.VMEM((2, 2, 2, side, columns), f32), pltpu.SemaphoreType.DMA((4 + 2 * len(outer),))],
        input_output_aliases={4: 0}, compiler_params=grant(57), name="edges",
    )(begin, old, halo[0], halo[1], nodes)


def power_of(row_base, rows, column_base, columns, size_x, size_y, doublings):
    real, imag, _ = rates(row_base, rows, column_base, columns, size_x, size_y)
    step_real = 1.0 - real
    step_imag = -imag
    share = 1.0 / (step_real * step_real + step_imag * step_imag)
    power = (step_real * share, -step_imag * share)
    first = power
    for _ in range(doublings):
        power = turned(power[0], power[1], power[0], power[1])
    return first, power


def step_kernel(total, field, out, *, doublings, rows, size_x, size_y, low_column):
    rank = lax.axis_index("space")
    coarse_rows, width = total.shape[1:]
    shift = jnp.where(rank >= lax.axis_size("space") // 2, 0, rows - coarse_rows)
    for start in range(0, coarse_rows, STRIP):
        here = pl.ds(start, STRIP)
        _, power = power_of(rank * rows + shift + start, STRIP, low_column, width, size_x, size_y, doublings)
        grown = turned(power[0], power[1], field[0, here, :], field[1, here, :])
        for part in range(2):
            out[part, here, :] = total[part, here, :] + grown[part]


def step_call(total, field, doublings, rows, size_x, size_y, low_column):
    kernel = functools.partial(step_kernel, doublings=doublings, rows=rows, size_x=size_x, size_y=size_y,
                               low_column=low_column)
    return pl.pallas_call(kernel, in_specs=[VMEM, VMEM], out_specs=VMEM,
                          out_shape=jax.ShapeDtypeStruct(total.shape, jnp.float32),
                          compiler_params=PARAMS, name="step")(total, field)


def patch_kernel(begin, nodes_in, outer_piece, *refs, doublings, coarse_rows, size_x, size_y, first_block):
    prior, received, offset, start, nodes = refs[-5:]
    rows = begin.shape[1]
    rank = lax.axis_index("space")
    ranks = lax.axis_size("space")
    lead = lax.axis_index("tm") == 0
    spot = pl.ds(pl.multiple_of(pl.program_id(0) * LANES, LANES), LANES)
    middle = jnp.logical_or(rank == ranks // 2, rank == ranks // 2 - 1)

    @pl.when(jnp.logical_not(middle))
    def _():
        nodes[...] = nodes_in[...]
        for part in range(2):
            start[part] = jnp.where(lead, begin[part], outer_piece[part, :, spot])

    def fix(shift):
        if rows > coarse_rows:
            other = pl.ds(0 if shift else coarse_rows, rows - coarse_rows)
            piece = refs[0]
            for part in range(2):
                start[part, other, :] = jnp.where(lead, begin[part, other, :], piece[part, :, spot])
                for k in range(2):
                    nodes[k, part, other, :] = nodes_in[k, part, other, :]
        for low in range(0, coarse_rows, STRIP):
            at = pl.ds(low, STRIP)
            here = pl.ds(shift + low, STRIP)
            first, power = power_of(rank * rows + shift + low, STRIP, (first_block + pl.program_id(0)) * LANES, LANES,
                                    size_x, size_y, doublings)
            grown = turned(power[0], power[1], received[0, at, spot], received[1, at, spot])
            total = [jnp.where(lead, 0.0, prior[part, at, spot] + grown[part]) for part in range(2)]
            carried = turned(first[0], first[1], total[0], total[1])
            for part in range(2):
                old_begin = begin[part, here, :]
                n2 = nodes_in[1, part, here, :]
                now = jnp.where(lead, old_begin, total[part])
                change = (offset[part, at, spot] + carried[part]) - n2
                nodes[0, part, here, :] = nodes_in[0, part, here, :] + 0.5 * ((now - old_begin) + change)
                nodes[1, part, here, :] = n2 + change
                start[part, here, :] = now

    if rows == coarse_rows:
        @pl.when(middle)
        def _():
            fix(0)
    else:
        @pl.when(rank == ranks // 2)
        def _():
            fix(0)

        @pl.when(rank == ranks // 2 - 1)
        def _():
            fix(rows - coarse_rows)


def patch_call(begin, nodes, arrived, scan, low_column, size_x, doublings):
    rows, columns = begin.shape[1:]
    base = low_column // LANES
    coarse_rows, width = scan[0].shape[1:]
    begin_spec = pl.BlockSpec((2, rows, LANES), lambda j: (0, 0, base + j))
    nodes_spec = pl.BlockSpec((2, 2, rows, LANES), lambda j: (0, 0, 0, base + j))
    kernel = functools.partial(patch_kernel, doublings=doublings, coarse_rows=coarse_rows, size_x=size_x,
                               size_y=columns, first_block=base)
    return pl.pallas_call(
        kernel, grid=(width // LANES,),
        in_specs=[begin_spec, nodes_spec] + [VMEM] * (len(arrived) + 3),
        out_specs=[begin_spec, nodes_spec],
        out_shape=[jax.ShapeDtypeStruct(begin.shape, jnp.float32), jax.ShapeDtypeStruct(nodes.shape, jnp.float32)],
        input_output_aliases={1: 1}, compiler_params=PARAMS, name="patch",
    )(begin, nodes, *arrived, *scan)


def place_kernel(begin, outer_part, middle_part, edges, _, start, *, spot):
    lead = lax.axis_index("tm") == 0
    rank = lax.axis_index("space")
    ranks = lax.axis_size("space")
    middle = jnp.logical_or(rank == ranks // 2, rank == ranks // 2 - 1)
    rows = begin.shape[1]
    here = pl.ds(pl.multiple_of(pl.program_id(0) * LANES, LANES), LANES)
    side = pl.ds(pl.multiple_of(spot + pl.program_id(0) * LANES, LANES), LANES)
    inside = pl.ds(PAD, rows - 2 * PAD)
    for part in range(2):
        start[part, pl.ds(0, PAD), :] = jnp.where(lead, begin[part, pl.ds(0, PAD), :], edges[part, pl.ds(0, PAD), side])
        start[part, pl.ds(rows - PAD, PAD), :] = jnp.where(
            lead, begin[part, pl.ds(rows - PAD, PAD), :], edges[part, pl.ds(PAD, PAD), side])

    @pl.when(middle)
    def _():
        for part in range(2):
            start[part, inside, :] = jnp.where(lead, begin[part, inside, :], middle_part[part, :, here])

    @pl.when(jnp.logical_not(middle))
    def _():
        for part in range(2):
            start[part, inside, :] = jnp.where(lead, begin[part, inside, :], outer_part[part, :, here])


def place_call(begin, outer_part, middle_part, edges, start, first, spot):
    rows = begin.shape[1]
    base = first // LANES
    spec = pl.BlockSpec((2, rows, LANES), lambda j: (0, 0, base + j))
    return pl.pallas_call(
        functools.partial(place_kernel, spot=spot), grid=(outer_part.shape[2] // LANES,),
        in_specs=[spec, VMEM, VMEM, VMEM, ANY], out_specs=spec,
        out_shape=jax.ShapeDtypeStruct(begin.shape, jnp.float32),
        input_output_aliases={4: 0}, compiler_params=PARAMS, name="place",
    )(begin, outer_part, middle_part, edges, start)


def body(start_values, node_values):
    begin = start_values[0]
    old = node_values[0]
    rows, columns = begin.shape[1:]
    slices, ranks = lax.axis_size("tm"), lax.axis_size("space")
    size_x = rows * ranks
    width = columns // COARSE_SHARE
    low_column = columns // 2 - width // 2
    coarse_rows = min(rows, size_x // COARSE_SHARE // 2)
    middle = (ranks // 2 - 1, ranks // 2)
    outer = [s for s in range(ranks) if s not in middle]
    everyone = range(ranks)

    def edge(low):
        cut = [begin[:, low:low + HALO], old[0, :, low:low + HALO], old[1, :, low:low + HALO]]
        return jnp.concatenate(cut, axis=0)

    up = [(i, i + 1) for i in range(ranks - 1)]
    before = lax.ppermute(edge(rows - HALO), "space", up)
    after = lax.ppermute(edge(0), "space", [(j, i) for i, j in up])

    def ahead(value, steps, members):
        pairs = [(n * ranks + s, (n + steps) * ranks + s) for n in range(slices - steps) for s in members]
        return lax.ppermute(value, ("tm", "space"), pairs)

    pieces = [(0, rows)] + ([(0, rows - coarse_rows)] if rows > coarse_rows else [])
    second = low_column + width
    rest = columns - second
    inside = [(PAD, rows - PAD)]
    nodes, left = fine_call(begin, old, None, None, 0, low_column, inside, size_x, coarse_rows, grant(62))
    left_outer = ahead(left, 1, outer)
    made = fine_call(begin, old, (before, after), nodes, low_column, width, pieces, size_x, coarse_rows, grant(60))
    nodes, inner_sends, offset = made[0], made[1:-1], made[-1]
    one_back = ahead(offset, 1, middle)
    two_back = ahead(offset, 2, middle)
    inner = [ahead(inner_sends[0], 1, outer)]
    left_middle = ahead(left, 1, middle)
    nodes, right = fine_call(begin, old, None, nodes, second, rest, inside, size_x, coarse_rows, grant(58))
    right_outer = ahead(right, 1, outer)
    nodes, edges = edge_call(begin, old, (before, after), nodes, [(0, low_column), (second, rest)], size_x)
    edges = ahead(edges, 1, everyone)
    inner += [ahead(piece, 1, middle) for piece in inner_sends[1:]]
    right_middle = ahead(right, 1, middle)

    total, field, reach, doublings = one_back, two_back, 1, 0
    while 2 * reach < slices:
        total = step_call(total, field, doublings, rows, size_x, columns, low_column)
        reach, doublings = 2 * reach, doublings + 1
        field = ahead(total, reach, middle)
    scan = (total, field, offset)
    next_start, nodes = patch_call(begin, nodes, inner, scan, low_column, size_x, doublings)
    next_start = place_call(begin, left_outer, left_middle, edges, next_start, 0, 0)
    next_start = place_call(begin, right_outer, right_middle, edges, next_start, second, low_column)
    return next_start[None], nodes[None]


def solution(mesh):
    in_specs = (P("tm", None, "space", None), P("tm", None, None, "space", None))
    out_specs = (P("tm", None, "space", None), P("tm", None, None, "space", None))
    return jax.shard_map(body, mesh=mesh, in_specs=in_specs, out_specs=out_specs, check_vma=False)
```
